32 devices in a mesh: mem: 8 (over z, y), hz: 4 (over x, core).
Axes of the slice: x: 2, y: 2, z: 4, core: 2. Of those that a mesh axis runs over, the one named last changes fastest.
Arguments:
- prior: float32 [8, 64, 32768], P('mem', None, 'hz'), may hold values from -6 to 6
- posterior: float32 [8, 64, 32768], P('mem', None, 'hz'), may hold values from -4 to 4
- control: float32 [64, 32768], P(None, 'hz'), may hold values from -6 to 6
- relax: float32 [64], replicated, may hold values from 0.5 to 0.95
- ocean: int32 [32768], P('hz'), may hold values 0 or 1
Outputs:
- analysis: float32 [8, 64, 32768], P('mem', None, 'hz')
The draws below stay inside these ranges and needn't reach their ends.
All inputs are finite; a program needn't handle non-finite values. No bound on the sum of `ocean` on one device may be relied on, other than what follows from the above.
Results may differ from the reference program's by a relative error of at most 0.00002.
Values sent between devices are 32-bit elements; how exact they have to be, the bound alone decides.
A program may use at most 64 MiB of HBM per device.

```python
import jax
import jax.numpy as jnp
from jax import lax

LEV = 64
MEMBERS = 8
NCOL = 32768


def touch_ends(drawn, rng, low, largest):
    dims = drawn.shape
    spot = [jax.random.randint(jax.random.fold_in(rng, axis), (), 0, dims[axis]) for axis in range(len(dims))]
    drawn = drawn.at[tuple(spot)].set(low)
    longest = dims.index(max(dims))
    spot[longest] = (spot[longest] + 1) % dims[longest]
    return drawn.at[tuple(spot)].set(largest)


def block_scale(key, shape, cuts, low, largest):
    def one(position, parts):
        draws = jax.random.uniform(jax.random.fold_in(jax.random.fold_in(key, 6), position), (parts,), jnp.float32, low / len(cuts), largest / len(cuts))
        return jnp.repeat(jnp.exp(draws), shape[position] // parts).reshape((-1,) + (1,) * (len(shape) - position - 1))

    loudness = one(*cuts[0])
    for cut in cuts[1:]:
        loudness = loudness * one(*cut)
    return loudness


def centred(key, dims, width, reach, shards=(), held_as=jnp.bfloat16):
    array = width * jax.random.normal(key, dims, jnp.float32)
    if shards:
        array = array * block_scale(key, dims, shards, -0.22, 0.18)
    return jnp.clip(array, -reach, reach).astype(held_as)


def setup_inputs(seed: int = 0) -> dict:
    key_of = jax.random.split(jax.random.key(seed), 6)
    prior = centred(key_of[0], (MEMBERS, LEV, NCOL), 1.0, 6.0, ((0, 8), (2, 4)), jnp.float32)
    posterior = centred(key_of[1], (MEMBERS, LEV, NCOL), 0.6, 4.0, ((0, 8), (2, 4)), jnp.float32)
    control = centred(key_of[2], (LEV, NCOL), 1.0, 6.0, ((1, 4),), jnp.float32)
    relax = jnp.clip(jax.random.uniform(key_of[3], (LEV,), jnp.float32, 0.5, 0.95), 0.5, 0.95)
    ocean = touch_ends((jax.random.randint(key_of[4], (NCOL,), 0, 4) < 3).astype(jnp.int32), jax.random.fold_in(key_of[4], 1), 0, 1)
    return {"prior": prior, "posterior": posterior, "control": control, "relax": relax, "ocean": ocean}


eps = 1e-06

def reference(prior, posterior, control, relax, ocean):
    prior_mean = lax.optimization_barrier(jnp.sum(prior, axis=0)) / MEMBERS
    post_mean = lax.optimization_barrier(jnp.sum(posterior, axis=0)) / MEMBERS
    weights = ocean.astype(jnp.float32)
    prior_anom = prior - prior_mean
    post_anom = posterior - post_mean
    prior_spread = lax.optimization_barrier(jnp.sum(prior_anom * prior_anom * weights, axis=(0, 2)))
    post_spread = lax.optimization_barrier(jnp.sum(post_anom * post_anom * weights, axis=(0, 2)))
    factor = relax * (jnp.sqrt((prior_spread + eps) / (post_spread + eps)) - 1.0) + 1.0
    return control + factor[None, :, None] * post_anom
```

```python
import functools

import jax
import jax.numpy as jnp
from jax import lax
from jax.experimental import pallas as pl
from jax.experimental.pallas import tpu as pltpu
from jax.sharding import PartitionSpec as P

eps = 1e-06
SUB = 8
LANE = 128
LAG = 2
MESH = pl.DeviceIdType.MESH
POST, PRIOR = 0, 1


def kernel(members, blocks, prior_hbm, post_hbm, control_hbm, relax_hbm, ocean_hbm, out,
           x, control, ocean, relax_ref, weights, total, y_in, pair, a_in, b_in, b_sum, b_swap, b_swap_prior, spread, part1, part2, zero,
           load_sem, control_sem, ocean_sem, relax_sem, y_send, y_recv, a_send, a_recv, b_send, b_recv, s_send, s_recv, p_send, p_recv,
           ga_send, ga_recv, gy_send, gy_recv, gb_send, gb_recv, h_send, h_recv, m_send, m_recv):
    levels, columns = control.shape
    half = columns // 2
    nblocks = levels // SUB
    quarter = nblocks // 4
    depth = members // 2
    m = lax.axis_index("mem")
    hz = lax.axis_index("hz")
    z = lax.div(m, 2)
    y = lax.rem(m, 2)
    other = 1 - y

    def device(zz, yy):
        return {"mem": zz * 2 + yy, "hz": hz}

    def rows(block):
        return pl.ds(pl.multiple_of(block * SUB, SUB), SUB)

    def cols(h):
        return pl.ds(pl.multiple_of(h * half, LANE), half)

    fields = (post_hbm, prior_hbm)

    def load(field, block):
        at = pl.ds(block * SUB, SUB)
        return pltpu.make_async_copy(fields[field].at[0, at], x.at[field, at], load_sem.at[field, block])

    barrier = pltpu.get_barrier_semaphore()

    def greet(to):
        pl.semaphore_signal(barrier, inc=1, device_id=to, device_id_type=MESH)

    greet(device(z, other))
    pl.when(z > 0)(lambda: greet(device(z - 1, y)))
    pl.when(z < depth - 1)(lambda: greet(device(z + 1, y)))
    for i in range(1, blocks):
        greet({"mem": m, "hz": lax.rem(hz + i, blocks)})

    ocean_load = pltpu.make_async_copy(ocean_hbm, ocean, ocean_sem)
    ocean_load.start()
    relax_load = pltpu.make_async_copy(relax_hbm, relax_ref, relax_sem)
    relax_load.start()
    order = []
    for i in range(2 * quarter):
        order += [i, 2 * quarter + i]
    for field in (POST, PRIOR):
        for block in order:
            load(field, block).start()
    control_load = pltpu.make_async_copy(control_hbm, control, control_sem)
    control_load.start()

    ocean_load.wait()
    weights[...] = jnp.broadcast_to(ocean[...].astype(jnp.float32), (SUB, columns))
    spread[...] = jnp.zeros_like(spread)
    pl.semaphore_wait(barrier, blocks + jnp.where(z > 0, 1, 0) + jnp.where(z < depth - 1, 1, 0))

    pending = []

    def send(src, dst, send_sem, recv_sem, to, cond=None):
        copy = pltpu.make_async_remote_copy(src_ref=src, dst_ref=dst, send_sem=send_sem, recv_sem=recv_sem,
                                            device_id=to, device_id_type=MESH)
        if cond is None:
            copy.start()
        else:
            pl.when(cond)(copy.start)
        pending.append((cond, copy))

    def arrive(dst, send_sem, recv_sem):
        pltpu.make_async_remote_copy(src_ref=dst, dst_ref=dst, send_sem=send_sem, recv_sem=recv_sem,
                                     device_id=device(z, other), device_id_type=MESH).wait_recv()

    def merge(own, n_own, came, n_came, dst, field, block, h, scale=None):
        n_own = jnp.float32(n_own)
        n_came = jnp.float32(n_came) if isinstance(n_came, int) else n_came.astype(jnp.float32)
        w = weights.at[:, cols(h)]
        acc = jnp.zeros((SUB, LANE), jnp.float32)
        for j in range(half // LANE):
            at = slice(j * LANE, (j + 1) * LANE)
            a, b = own[:, at], came[:, at]
            d = b * n_own - a * n_came
            acc += d * d * w[:, at]
            if dst is not None:
                dst[:, at] = a + b
        acc = acc / jnp.full((SUB, LANE), n_own * n_came * (n_own + n_came), jnp.float32)
        if scale is not None:
            acc = acc * scale
        spread[field, block] += acc

    up_near = 2 * z < depth
    near = jnp.where(up_near, 0, 1)
    far = 1 - near

    def place(d):
        at = jnp.where(d == 0, z, depth - 1 - z)
        return at, z + 1 - 2 * d, z - 1 + 2 * d

    def first(field):
        for block in order:
            load(field, block).wait()
        for d in (near, far):
            for k in range(quarter):
                i = d * quarter + k
                send(x.at[field, rows(i), cols(other)], y_in.at[field, i], y_send.at[field, i], y_recv.at[field, i],
                     device(z, other))

    def start_b(field):
        at, nxt, _ = place(near)
        for k in range(quarter):
            for h in range(2):
                i = near * quarter + k
                send(x.at[field, rows(2 * quarter + i), pl.ds(h * half, half)], b_in.at[field, i, h],
                     b_send.at[field, i, h], b_recv.at[field, i, h], device(nxt, y), (at == 0) & (at < depth - 1))

    def pair_step(field, d, k):
        at, nxt, _ = place(d)
        i = d * quarter + k
        mine = pair.at[field, i]
        arrive(y_in.at[field, i], y_send.at[field, i], y_recv.at[field, i])
        merge(x.at[field, rows(i), cols(y)], 1, y_in.at[field, i], 1, mine, field, i, y)
        send(mine, a_in.at[field, i], a_send.at[field, i], a_recv.at[field, i], device(nxt, y), (at == 0) & (at < depth - 1))

    def a_step(field, d, k):
        at, nxt, back = place(d)
        i = d * quarter + k
        mine = pair.at[field, i]

        @pl.when(at > 0)
        def _():
            arrive(a_in.at[field, i], a_send.at[field, i], a_recv.at[field, i])
            merge(mine, 2, a_in.at[field, i], 2 * at, mine, field, i, y)

        send(mine, a_in.at[field, i], a_send.at[field, i], a_recv.at[field, i], device(nxt, y), (at > 0) & (at < depth - 1))
        if field == POST:
            last = at == depth - 1
            spot = total.at[rows(i), cols(y)]

            @pl.when(last)
            def _():
                spot[...] = mine[...]

            send(mine, spot, ga_send.at[i], ga_recv.at[i], device(back, y), last & (at > 0))
            send(mine, spot, gy_send.at[i], gy_recv.at[i], device(z, other), last)

    def b_step(field, d, k, h):
        at, nxt, _ = place(d)
        i = d * quarter + k
        block = 2 * quarter + i
        own = x.at[field, rows(block), cols(h)]
        mine = b_sum.at[field, i, h]

        @pl.when(at > 0)
        def _():
            arrive(b_in.at[field, i, h], b_send.at[field, i, h], b_recv.at[field, i, h])
            merge(own, 1, b_in.at[field, i, h], at, mine, field, block, h)

        last = at == depth - 1
        send(mine, b_in.at[field, i, h], b_send.at[field, i, h], b_recv.at[field, i, h], device(nxt, y), (at > 0) & ~last)
        if field == POST:
            send(mine, b_swap.at[i, h], s_send.at[i, h], s_recv.at[i, h], device(z, other), last)
        else:
            send(mine, b_swap_prior.at[i], p_send.at[i], p_recv.at[i], device(z, other), last & (other == h))

    def swap_step(d, k, h):
        at, _, back = place(d)
        i = d * quarter + k
        block = 2 * quarter + i
        last = at == depth - 1
        spot = total.at[rows(block), pl.ds(h * half, half)]

        @pl.when(last)
        def _():
            arrive(b_swap.at[i, h], s_send.at[i, h], s_recv.at[i, h])
            merge(b_sum.at[POST, i, h], depth, b_swap.at[i, h], depth, spot, POST, block, h, jnp.where(y == h, 1.0, 0.0))

        send(spot, spot, gb_send.at[i, h], gb_recv.at[i, h], device(back, y), last & (at > 0))

    def swap_prior(d, k):
        at, _, _ = place(d)
        i = d * quarter + k

        @pl.when(at == depth - 1)
        def _():
            arrive(b_swap_prior.at[i], p_send.at[i], p_recv.at[i])
            merge(b_sum.at[PRIOR, i, y], depth, b_swap_prior.at[i], depth, None, PRIOR, 2 * quarter + i, y)

    def a_relay(d, k):
        at, _, back = place(d)
        i = d * quarter + k
        spot = total.at[rows(i), cols(y)]
        below = at < depth - 1

        @pl.when(below)
        def _():
            arrive(spot, ga_send.at[i], ga_recv.at[i])

        send(spot, spot, ga_send.at[i], ga_recv.at[i], device(back, y), below & (at > 0))
        send(spot, spot, gy_send.at[i], gy_recv.at[i], device(z, other), below)

    def b_relay(d, k, h):
        at, _, back = place(d)
        i = d * quarter + k
        spot = total.at[rows(2 * quarter + i), pl.ds(h * half, half)]
        below = at < depth - 1

        @pl.when(below)
        def _():
            arrive(spot, gb_send.at[i, h], gb_recv.at[i, h])

        send(spot, spot, gb_send.at[i, h], gb_recv.at[i, h], device(back, y), below & (at > 0))

    first(POST)
    start_b(POST)
    first(PRIOR)

    def chain(field):
        steps = []
        for k in range(quarter):
            for h in range(2):
                steps.append(functools.partial(lambda k, h, d: b_step(field, d, k, h), k, h))
        for k in range(quarter):
            steps.append(functools.partial(lambda k, d: a_step(field, d, k), k))
        return steps

    post_steps, prior_steps = chain(POST), chain(PRIOR)
    nb = 2 * quarter
    pairs = [(field, d, k) for field in (POST, PRIOR) for d in (near, far) for k in range(quarter)]
    swaps = [functools.partial(lambda k, h, d: swap_step(d, k, h), k, h) for k in range(quarter) for h in range(2)]
    steps = post_steps + prior_steps
    n = len(steps)
    units = [(None, k) for k in range(quarter)] + [(h, k) for k in range(quarter) for h in range(2)]

    def relay(d, h, k):
        if h is None:
            a_relay(d, k)
        else:
            b_relay(d, k, h)

    events = []
    for u in range(len(units) + 1):
        if u < len(units):
            events.append((far, *units[u]))
        if u >= 1:
            events.append((near, *units[u - 1]))
    cut1, cut2 = len(events) // 3, 2 * len(events) // 3
    done_pairs = 0
    for s in range(n + LAG):
        if done_pairs < len(pairs):
            pair_step(*pairs[done_pairs])
            done_pairs += 1
            if done_pairs == quarter:
                start_b(PRIOR)
        if s < n:
            steps[s](near)
        if s >= LAG:
            steps[s - LAG](far)
        t = s - LAG - nb - 1
        if 0 <= t < len(swaps):
            swaps[t](0)
            swaps[t](1)
        if s == n + LAG - 2:
            relay(*events[0])
    for k in range(quarter):
        swap_prior(0, k)
        swap_prior(1, k)

    lane = lax.broadcasted_iota(jnp.int32, (SUB, LANE), 1)
    for field in (POST, PRIOR):
        packed = jnp.zeros((SUB, LANE), jnp.float32)
        for block in range(nblocks):
            packed = jnp.where(lane == block, jnp.sum(spread[field, block], axis=1, keepdims=True), packed)
        part1[hz, field] = packed
    for i in range(1, blocks):
        send(part1.at[hz], part1.at[hz], h_send.at[i], h_recv.at[hz], {"mem": m, "hz": lax.rem(hz + i, blocks)})

    for event in events[1:cut1]:
        relay(*event)
    for i in range(1, blocks):
        src = lax.rem(hz + i, blocks)
        arrive(part1.at[src], h_send.at[i], h_recv.at[src])
    for field in (POST, PRIOR):
        v = part1[0, field]
        for i in range(1, blocks):
            v = v + part1[i, field]
        part2[m, field] = v
    for i in range(1, members):
        send(part2.at[m], part2.at[m], m_send.at[i], m_recv.at[m], {"mem": lax.rem(m + i, members), "hz": hz})
    for event in events[cut1:cut2]:
        relay(*event)
    for i in range(1, members):
        src = lax.rem(m + i, members)
        arrive(part2.at[src], m_send.at[i], m_recv.at[src])
    spreads = []
    for field in (POST, PRIOR):
        v = part2[0, field]
        for i in range(1, members):
            v = v + part2[i, field]
        spreads.append(v)
    sub = lax.broadcasted_iota(jnp.int32, (SUB, LANE), 0)
    relax_load.wait()
    relax = jnp.zeros((SUB, LANE), jnp.float32)
    for level in range(levels):
        relax = jnp.where((sub == level % SUB) & (lane == level // SUB), relax_ref[level], relax)
    factor = relax * (jnp.sqrt((spreads[PRIOR] + eps) / (spreads[POST] + eps)) - 1.0) + 1.0
    for block in range(nblocks):
        zero[block] = jnp.broadcast_to(
            jnp.sum(jnp.where(lane == block, factor, 0.0), axis=1, keepdims=True), (SUB, LANE))
    control_load.wait()

    def finish(block, h):
        f = zero[block]
        c, p, t, o = (r.at[rows(block), cols(h)] for r in (control, x.at[POST], total, out.at[0]))
        for j in range(half // LANE):
            at = slice(j * LANE, (j + 1) * LANE)
            o[:, at] = c[:, at] + f * (p[:, at] - t[:, at] / members)

    for i, (d, h, k) in enumerate(events):
        if i >= cut2:
            relay(d, h, k)
        if h is None:
            finish(d * quarter + k, y)
        else:
            finish(2 * quarter + d * quarter + k, h)
    for k in range(quarter):
        for d in (near, far):
            i = d * quarter + k
            arrive(total.at[rows(i), cols(other)], gy_send.at[i], gy_recv.at[i])
            finish(i, other)
    for cond, copy in pending:
        if cond is None:
            copy.wait_send()
        else:
            pl.when(cond)(copy.wait_send)


def solution(mesh):
    members, blocks = mesh.shape["mem"], mesh.shape["hz"]

    def on_device(prior, posterior, control, relax, ocean):
        levels, columns = control.shape
        half, nblocks = columns // 2, levels // SUB
        a, q = nblocks // 2, nblocks // 4
        vmem = lambda *shape: pltpu.VMEM(shape, jnp.float32)
        dma = lambda *shape: pltpu.SemaphoreType.DMA(shape)
        hbm = pl.BlockSpec(memory_space=pltpu.HBM)
        return pl.pallas_call(
            functools.partial(kernel, members, blocks),
            out_shape=pltpu.VMEM(posterior.shape, jnp.float32),
            in_specs=[hbm] * 5,
            out_specs=pl.BlockSpec(memory_space=pltpu.VMEM),
            scratch_shapes=[
                vmem(2, levels, columns), vmem(levels, columns), pltpu.VMEM((1, columns), jnp.int32),
                pltpu.SMEM((levels,), jnp.float32), vmem(SUB, columns), vmem(levels, columns), vmem(2, a, SUB, half), vmem(2, a, SUB, half), vmem(2, a, SUB, half),
                vmem(2, a, 2, SUB, half), vmem(2, a, 2, SUB, half), vmem(a, 2, SUB, half), vmem(a, SUB, half),
                vmem(2, nblocks, SUB, LANE), vmem(blocks, 2, SUB, LANE), vmem(members, 2, SUB, LANE),
                vmem(nblocks, SUB, LANE),
                dma(2, nblocks), pltpu.SemaphoreType.DMA, pltpu.SemaphoreType.DMA, pltpu.SemaphoreType.DMA,
                dma(2, a), dma(2, a), dma(2, a), dma(2, a), dma(2, a, 2), dma(2, a, 2), dma(a, 2), dma(a, 2), dma(a), dma(a),
                dma(a), dma(a), dma(a), dma(a), dma(a, 2), dma(a, 2), dma(blocks), dma(blocks), dma(members), dma(members),
            ],
            compiler_params=pltpu.CompilerParams(
                collective_id=0, has_side_effects=True, vmem_limit_bytes=60 * 2**20
            ),
        )(prior, posterior, control, relax, ocean.reshape(1, columns))

    return jax.shard_map(
        on_device,
        mesh=mesh,
        in_specs=(P("mem", None, "hz"), P("mem", None, "hz"), P(None, "hz"), P(), P("hz")),
        out_specs=P("mem", None, "hz"),
        check_vma=False,
    )
```

```python
import functools

import jax
import jax.numpy as jnp
from jax import lax
from jax.experimental import pallas as pl
from jax.experimental.pallas import tpu as pltpu
from jax.sharding import PartitionSpec as P

eps = 1e-06
SUB = 8
LANE = 128
MESH = pl.DeviceIdType.MESH
POST, PRIOR = 0, 1
ROWS_FIRST, DEPTH_FIRST = 0, 1
NEAR, FAR = 0, 1
PAIRS = 4
SHARE = 0.34375

(Y_SEND, Y_RECV, RS_IN, RS_OUT, RS_FROM_OUT, RS_FROM_IN, SW_SEND, SW_RECV,
 AG_IN, AG_OUT, AG_FROM_OUT, AG_FROM_IN, AGY_SEND, AGY_RECV, STAT1, STAT2, STAT3) = range(17)

MIDDLE = ((0, 1, 2), (0, 1, 3), (1, 0, 2))
ORDER_END = (
    0, 73, 91, 3, 77, 1, 32, 89, 2, 35, 67, 6, 33, 65, 5, 34, 76, 168, 200, 38, 95, 4, 186, 37, 69, 7, 232, 93, 184, 23,
    36, 75, 17, 162, 39, 71, 218, 160, 55, 87, 216, 19, 49, 81, 190, 250, 16, 248, 78, 364, 222, 51, 83, 386, 164, 48,
    260, 22, 188, 254, 79, 170, 202, 418, 256, 21, 365, 54, 220, 166, 262, 234, 20, 258, 182, 53, 388, 252, 85, 176, 18,
    52, 84, 384, 420, 266, 357, 389, 50, 178, 448, 264, 353, 385, 416, 359, 391, 421, 355, 387, 417, 480, 366, 390, 423,
    367, 419, 512, 363, 422, 361,
)
ORDER_INNER = (
    0, 3, 1, 137, 73, 32, 2, 155, 91, 35, 141, 77, 6, 168, 104, 33, 153, 89, 5, 186, 122, 34, 131, 67, 4, 38, 184, 120,
    129, 65, 7, 37, 140, 172, 162, 98, 23, 36, 159, 95, 160, 96, 204, 39, 133, 69, 17, 55, 157, 93, 190, 126, 19, 236,
    300, 139, 75, 164, 16, 49, 100, 268, 135, 188, 22, 51, 71, 124, 151, 170, 21, 48, 106, 87, 365, 145, 20, 301, 54,
    81, 142, 166, 18, 102, 53, 147, 83, 182, 118, 52, 324, 388, 260, 176, 112, 50, 143, 79, 178, 114, 320, 384, 256,
    420, 357, 293, 389, 326, 262, 174, 206, 416, 322, 258, 353, 289, 386, 421, 149, 85, 359, 295, 391, 238, 270, 148,
    355, 291, 387, 302, 418, 330, 266, 180, 448, 385, 328, 264, 423, 367, 303, 480, 390, 363, 299, 419, 361, 297, 417,
    512, 422,
)


def decode(step):
    step, side = divmod(step, 2)
    step, k = divmod(step, PAIRS)
    step, cls = divmod(step, 2)
    op, field = divmod(step, 2)
    return op, field, cls, k, side


def when(cond, do):
    if isinstance(cond, bool):
        if cond:
            do()
    else:
        pl.when(cond)(do)


def kernel(members, blocks, wide, prior_hbm, post_hbm, control_hbm, relax_hbm, ocean_hbm, out,
           x, control, ocean, relax_ref, weights, total, y_in, a_sum, a_in, b_sum, b_in, b_swap, spread, part1, part2, factors,
           load_sem, control_sem, ocean_sem, relax_sem, y_send, y_recv, a_send, a_recv, b_send, b_recv, w_send, w_recv,
           ga_send, ga_recv, gb_send, gb_recv, gy_send, gy_recv, h_send, h_recv, m_send, m_recv):
    levels, columns = control.shape
    nblocks = levels // SUB
    pairs = nblocks // 2
    rest = columns - 2 * wide
    half = rest // 2
    depth = members // 2
    m = lax.axis_index("mem")
    hz = lax.axis_index("hz")
    z = lax.div(m, 2)
    y = lax.rem(m, 2)
    other = 1 - y
    upper = z >= depth // 2
    up = jnp.where(upper, 1, 0)
    inward = jnp.where(upper, z - 1, z + 1)
    outward = jnp.where(upper, z + 1, z - 1)
    distance = jnp.where(upper, depth - 1 - z, z)
    center = depth // 2 - 1
    to_in, to_out = up, 1 - up

    def device(zz, yy):
        return {"mem": zz * 2 + yy, "hz": hz}

    barrier = pltpu.get_barrier_semaphore()

    def greet(to):
        pl.semaphore_signal(barrier, inc=1, device_id=to, device_id_type=MESH)

    greet(device(z, other))
    greet(device(inward, y))
    pl.when(distance > 0)(lambda: greet(device(outward, y)))
    for i in range(1, blocks):
        greet({"mem": m, "hz": lax.rem(hz + i, blocks)})

    def block_of(k, side):
        return k + pairs * (up if side == NEAR else 1 - up)

    def rows(block):
        return pl.ds(pl.multiple_of(block * SUB, SUB), SUB)

    def wide_cols(yy):
        return pl.ds(pl.multiple_of(yy * wide, LANE), wide)

    rest_cols = pl.ds(2 * wide, rest)
    fields = (post_hbm, prior_hbm)

    def load(field, block):
        return pltpu.make_async_copy(fields[field].at[0, rows(block)], x.at[field, rows(block)], load_sem.at[field, block])

    for field in (POST, PRIOR):
        for k in range(pairs):
            for side in (FAR, NEAR):
                load(field, block_of(k, side)).start()
    ocean_load = pltpu.make_async_copy(ocean_hbm, ocean, ocean_sem)
    ocean_load.start()
    control_load = pltpu.make_async_copy(control_hbm, control, control_sem)
    control_load.start()
    relax_load = pltpu.make_async_copy(relax_hbm, relax_ref, relax_sem)
    relax_load.start()
    spread[...] = jnp.zeros_like(spread)
    ocean_load.wait()
    weights[...] = jnp.broadcast_to(ocean[...].astype(jnp.float32), (SUB, columns))
    pl.semaphore_wait(barrier, 1 + blocks + jnp.where(distance > 0, 1, 0))

    def arrive(dst, send_sem, recv_sem):
        pltpu.make_async_remote_copy(src_ref=dst, dst_ref=dst, send_sem=send_sem, recv_sem=recv_sem,
                                     device_id=device(z, other), device_id_type=MESH).wait_recv()

    def merge(own, n_own, came, n_came, w, dst, field, block, scale=1.0):
        acc = jnp.zeros((SUB, LANE), jnp.float32)
        static = isinstance(n_own, int) and isinstance(n_came, int)
        equal = static and n_own == n_came
        if not static:
            f_own, f_came = (jnp.float32(n) if isinstance(n, int) else n.astype(jnp.float32) for n in (n_own, n_came))
        for j in range(own.shape[-1] // LANE):
            at = slice(j * LANE, (j + 1) * LANE)
            a, b = own[:, at], came[:, at]
            if equal:
                d = b - a
            elif static:
                d = b * float(n_own) - a * float(n_came)
            else:
                d = b * f_own - a * f_came
            acc += d * d * w[:, at]
            if dst is not None:
                dst[:, at] = a + b
        if equal:
            acc = acc * (scale / (2 * n_own))
        elif static:
            acc = acc * (scale / (n_own * n_came * (n_own + n_came)))
        else:
            acc = acc / jnp.full((SUB, LANE), f_own * f_came * (f_own + f_came), jnp.float32) * scale
        spread[field, block] += acc

    lane = lax.broadcasted_iota(jnp.int32, (SUB, LANE), 1)
    sub = lax.broadcasted_iota(jnp.int32, (SUB, LANE), 0)

    def role(order, end):
        pending = []
        loaded = set()
        finished = []
        state = {"factor": False}
        far = 0 if end else (1 if center == 1 else distance)
        at_center = False if end else (True if center == 1 else distance == center)
        before = False if end else (False if center == 1 else distance < center)
        last_step = {}
        for i, step in enumerate(order):
            op, *chunk = decode(step)
            if op in (AG_OUT, AGY_SEND):
                last_step[tuple(chunk)] = i

        def send(src, dst, send_sem, recv_sem, to, cond=True):
            copy = pltpu.make_async_remote_copy(src_ref=src, dst_ref=dst, send_sem=send_sem, recv_sem=recv_sem,
                                                device_id=to, device_id_type=MESH)
            when(cond, copy.start)
            pending.append((cond, copy))

        def local(field, k, side):
            block = block_of(k, side)
            if (field, k, side) not in loaded:
                loaded.add((field, k, side))
                load(field, block).wait()
            return block

        def chain_send(field, cls, k, side, direction, to, cond=True):
            block = local(field, k, side)
            if cls == ROWS_FIRST:
                src, came, send_sem, recv_sem = a_sum.at[field, block], a_in, a_send, a_recv
            else:
                first = end and (side == FAR or (field, cls, k) in MIDDLE)
                src = x.at[field, rows(block), rest_cols] if first else b_sum.at[field, block]
                came, send_sem, recv_sem = b_in, b_send, b_recv
            at = (field, block, direction)
            send(src, came.at[at], send_sem.at[at], recv_sem.at[at], to, cond)

        def chain_merge(field, cls, k, side, direction, n_before, n_came, dst=True):
            block = local(field, k, side)
            at = (field, block, direction)
            if cls == ROWS_FIRST:
                came, own, w = a_in, a_sum.at[field, block], weights.at[:, wide_cols(y)]
                arrive(came.at[at], a_send.at[at], a_recv.at[at])
                into = {True: own, None: None, "total": total.at[rows(block), wide_cols(y)]}[dst]
                merge(own, 2 * n_before, came.at[at], 2 * n_came, w, into, field, block)
            else:
                came, w = b_in, weights.at[:, rest_cols]
                own = x.at[field, rows(block), rest_cols] if isinstance(n_before, int) and n_before == 1 else b_sum.at[field, block]
                arrive(came.at[at], b_send.at[at], b_recv.at[at])
                merge(own, n_before, came.at[at], n_came, w, b_sum.at[field, block], field, block)

        def spot(cls, block):
            return total.at[rows(block), wide_cols(y) if cls == ROWS_FIRST else rest_cols]

        def total_send(cls, block, direction, to, cond=True):
            s, r = (ga_send, ga_recv) if cls == ROWS_FIRST else (gb_send, gb_recv)
            at = (block, direction)
            send(spot(cls, block), spot(cls, block), s.at[at], r.at[at], to, cond)

        def total_arrive(cls, block, direction):
            s, r = (ga_send, ga_recv) if cls == ROWS_FIRST else (gb_send, gb_recv)
            at = (block, direction)
            arrive(spot(cls, block), s.at[at], r.at[at])

        def finish(block, cols):
            f = factors[block]
            c, p, t, o = (r.at[rows(block), cols] for r in (control, x.at[POST], total, out.at[0]))
            for j in range(c.shape[-1] // LANE):
                at = slice(j * LANE, (j + 1) * LANE)
                o[:, at] = c[:, at] + f * (p[:, at] - t[:, at] / members)

        def ready(block, cols):
            if state["factor"]:
                finish(block, cols)
            else:
                finished.append((block, cols))

        for i, step in enumerate(order):
            op, field, cls, k, side = decode(step)
            middle = (field, cls, k) in MIDDLE
            dst_total = "total" if cls == ROWS_FIRST and field == POST else None
            if op < STAT1:
                block = block_of(k, side)
                root_here = side == NEAR and (end != middle)
            if op == Y_SEND:
                local(field, k, side)
                send(x.at[field, rows(block), wide_cols(other)], y_in.at[field, block],
                     y_send.at[field, block], y_recv.at[field, block], device(z, other))
            elif op == Y_RECV:
                local(field, k, side)
                arrive(y_in.at[field, block], y_send.at[field, block], y_recv.at[field, block])
                merge(x.at[field, rows(block), wide_cols(y)], 1, y_in.at[field, block], 1, weights.at[:, wide_cols(y)],
                      a_sum.at[field, block], field, block)
            elif op == RS_IN:
                chain_send(field, cls, k, side, to_in, device(inward, y))
            elif op == RS_OUT:
                chain_send(field, cls, k, side, to_out, device(outward, y))
            elif op == RS_FROM_OUT:
                if side == FAR or not middle:
                    chain_merge(field, cls, k, side, to_in, 1, far)
                else:
                    chain_merge(field, cls, k, side, to_in, 1, far)
                    if before is not False:
                        chain_send(field, cls, k, side, to_in, device(inward, y), before)
            elif op == RS_FROM_IN:
                if end:
                    chain_merge(field, cls, k, side, to_out, 1, depth - 1, dst_total if cls == ROWS_FIRST else True)
                elif not middle:
                    chain_merge(field, cls, k, side, to_out, 1, depth - 1 - far)
                else:
                    when(at_center, lambda: chain_merge(field, cls, k, side, to_out, far + 1, depth - 1 - far,
                                                        dst_total if cls == ROWS_FIRST else True))
                if cls == ROWS_FIRST and field == POST and root_here and before is False:
                    ready(block, wide_cols(y))
            elif op == SW_SEND:
                cond = True if end else at_center
                if field == POST:
                    send(b_sum.at[POST, block], b_swap.at[POST, block], w_send.at[POST, block], w_recv.at[POST, block],
                         device(z, other), cond)
                else:
                    send(b_sum.at[PRIOR, block, :, pl.ds(pl.multiple_of(other * half, LANE), half)],
                         b_swap.at[PRIOR, block, :, pl.ds(0, half)],
                         w_send.at[PRIOR, block], w_recv.at[PRIOR, block], device(z, other), cond)
            elif op == SW_RECV:
                cond = True if end else at_center
                if field == POST:
                    def do(block=block):
                        arrive(b_swap.at[POST, block], w_send.at[POST, block], w_recv.at[POST, block])
                        merge(b_sum.at[POST, block], depth, b_swap.at[POST, block], depth, weights.at[:, rest_cols],
                              spot(DEPTH_FIRST, block), POST, block, 0.5)
                    when(cond, do)
                    if before is False:
                        ready(block, rest_cols)
                else:
                    def do(block=block):
                        mine = pl.ds(pl.multiple_of(y * half, LANE), half)
                        came = b_swap.at[PRIOR, block, :, pl.ds(0, half)]
                        arrive(came, w_send.at[PRIOR, block], w_recv.at[PRIOR, block])
                        merge(b_sum.at[PRIOR, block, :, mine], depth, came, depth,
                              weights.at[:, pl.ds(pl.multiple_of(2 * wide + y * half, LANE), half)], None, PRIOR, block)
                    when(cond, do)
            elif op == AG_IN:
                total_send(cls, block, to_in, device(inward, y), at_center if root_here and not end else True)
            elif op in (AG_OUT, AGY_SEND):
                cond = at_center if root_here and not end else True
                if op == AG_OUT:
                    total_send(cls, block, to_out, device(outward, y), cond)
                else:
                    send(spot(cls, block), spot(cls, block), gy_send.at[block], gy_recv.at[block], device(z, other), cond)
                if root_here and before is not False and last_step[field, cls, k, side] == i:
                    def do(cls=cls, block=block):
                        total_arrive(cls, block, to_out)
                    when(before, do)
                    total_send(cls, block, to_out, device(outward, y), before)
                    if cls == ROWS_FIRST:
                        send(spot(cls, block), spot(cls, block), gy_send.at[block], gy_recv.at[block], device(z, other), before)
                    ready(block, wide_cols(y) if cls == ROWS_FIRST else rest_cols)
            elif op == AG_FROM_OUT:
                total_arrive(cls, block, to_in)
                ready(block, wide_cols(y) if cls == ROWS_FIRST else rest_cols)
            elif op == AG_FROM_IN:
                total_arrive(cls, block, to_out)
                ready(block, wide_cols(y) if cls == ROWS_FIRST else rest_cols)
            elif op == AGY_RECV:
                arrive(total.at[rows(block), wide_cols(other)], gy_send.at[block], gy_recv.at[block])
                ready(block, wide_cols(other))
            elif op == STAT1:
                for field in (POST, PRIOR):
                    packed = jnp.zeros((SUB, LANE), jnp.float32)
                    for b in range(nblocks):
                        packed = jnp.where(lane == b, jnp.sum(spread[field, b], axis=1, keepdims=True), packed)
                    part1[hz, field] = packed
                for b in range(1, blocks):
                    send(part1.at[hz], part1.at[hz], h_send.at[b], h_recv.at[hz], {"mem": m, "hz": lax.rem(hz + b, blocks)})
            elif op == STAT2:
                for b in range(1, blocks):
                    src = lax.rem(hz + b, blocks)
                    arrive(part1.at[src], h_send.at[b], h_recv.at[src])
                for field in (POST, PRIOR):
                    v = part1[0, field]
                    for b in range(1, blocks):
                        v = v + part1[b, field]
                    part2[m, field] = v
                for b in range(1, members):
                    send(part2.at[m], part2.at[m], m_send.at[b], m_recv.at[m], {"mem": lax.rem(m + b, members), "hz": hz})
            elif op == STAT3:
                for b in range(1, members):
                    src = lax.rem(m + b, members)
                    arrive(part2.at[src], m_send.at[b], m_recv.at[src])
                sums = []
                for field in (POST, PRIOR):
                    v = part2[0, field]
                    for b in range(1, members):
                        v = v + part2[b, field]
                    sums.append(v)
                relax_load.wait()
                relax = jnp.zeros((SUB, LANE), jnp.float32)
                for level in range(levels):
                    relax = jnp.where((sub == level % SUB) & (lane == level // SUB), relax_ref[level], relax)
                factor = relax * (jnp.sqrt((sums[PRIOR] + eps) / (sums[POST] + eps)) - 1.0) + 1.0
                for b in range(nblocks):
                    factors[b] = jnp.broadcast_to(
                        jnp.sum(jnp.where(lane == b, factor, 0.0), axis=1, keepdims=True), (SUB, LANE))
                control_load.wait()
                state["factor"] = True
            if state["factor"] and finished:
                for _ in range(2):
                    if finished:
                        finish(*finished.pop(0))
        for todo in finished:
            finish(*todo)
        for cond, copy in pending:
            when(cond, copy.wait_send)

    @pl.when(distance == 0)
    def _():
        role(ORDER_END, True)

    @pl.when(distance > 0)
    def _():
        role(ORDER_INNER, False)


def solution(mesh):
    members, blocks = mesh.shape["mem"], mesh.shape["hz"]

    def on_device(prior, posterior, control, relax, ocean):
        levels, columns = control.shape
        n = levels // SUB
        wide = round(columns * SHARE / LANE) * LANE
        rest = columns - 2 * wide
        vmem = lambda *shape: pltpu.VMEM(shape, jnp.float32)
        dma = lambda *shape: pltpu.SemaphoreType.DMA(shape)
        one = pltpu.SemaphoreType.DMA
        return pl.pallas_call(
            functools.partial(kernel, members, blocks, wide),
            out_shape=pltpu.VMEM(posterior.shape, jnp.float32),
            in_specs=[pl.BlockSpec(memory_space=pltpu.HBM)] * 5,
            out_specs=pl.BlockSpec(memory_space=pltpu.VMEM),
            scratch_shapes=[
                vmem(2, levels, columns), vmem(levels, columns), pltpu.VMEM((1, columns), jnp.int32),
                pltpu.SMEM((levels,), jnp.float32), vmem(SUB, columns), vmem(levels, columns),
                vmem(2, n, SUB, wide), vmem(2, n, SUB, wide), vmem(2, n, 2, SUB, wide),
                vmem(2, n, SUB, rest), vmem(2, n, 2, SUB, rest), vmem(2, n, SUB, rest),
                vmem(2, n, SUB, LANE), vmem(blocks, 2, SUB, LANE), vmem(members, 2, SUB, LANE), vmem(n, SUB, LANE),
                dma(2, n), one, one, one, dma(2, n), dma(2, n), dma(2, n, 2), dma(2, n, 2), dma(2, n, 2), dma(2, n, 2),
                dma(2, n), dma(2, n), dma(n, 2), dma(n, 2), dma(n, 2), dma(n, 2), dma(n), dma(n),
                dma(blocks), dma(blocks), dma(members), dma(members),
            ],
            compiler_params=pltpu.CompilerParams(
                collective_id=0, has_side_effects=True, vmem_limit_bytes=60 * 2**20
            ),
        )(prior, posterior, control, relax, ocean.reshape(1, columns))

    return jax.shard_map(
        on_device,
        mesh=mesh,
        in_specs=(P("mem", None, "hz"), P("mem", None, "hz"), P(None, "hz"), P(), P("hz")),
        out_specs=P("mem", None, "hz"),
        check_vma=False,
    )
```

```python
import functools
import math

import jax
import jax.numpy as jnp
from jax import lax
from jax.experimental import pallas as pl
from jax.experimental.pallas import tpu as pltpu
from jax.sharding import PartitionSpec as P

eps = 1e-06
SUB = 8
LANE = 128
MESH = pl.DeviceIdType.MESH
POST, PRIOR = 0, 1
ROWS_FIRST, DEPTH_FIRST = 0, 1
NEAR, FAR = 0, 1
PAIRS = 4
SHORT_LINE = 4

(Y_SEND, Y_RECV, RS_IN, RS_OUT, RS_FROM_OUT, RS_FROM_IN, SW_SEND, SW_RECV, AG_IN, AG_OUT, AG_RECV,
 AGY_SEND, AGY_RECV, V_SEND, V_RECV, W_SEND, W_RECV, STAT1, STAT2, STAT3) = range(20)

PLAN = {
    "share": 0.375,
    "split": 1,
    "middle": ((0, 1, 1), (0, 1, 2), (0, 1, 3), (1, 0, 3)),
    "via": {(1, 0, 1): 1, (1, 1, 0): 1, (1, 1, 1): 1, (1, 2, 0): 1, (1, 2, 1): 1, (1, 3, 1): 1},
    "end": (
        181, 13, 177, 5, 157, 149, 9, 77, 929, 141, 32, 69, 936, 185, 40, 156, 73, 937, 1, 137, 96, 933, 12, 189, 104,
        941, 145, 37, 368, 148, 65, 432, 129, 932, 33, 76, 372, 133, 41, 101, 496, 165, 332, 8, 376, 97, 524, 4, 668,
        105, 169, 0, 72, 328, 520, 380, 444, 336, 400, 68, 161, 45, 669, 64, 153, 508, 320, 704, 512, 464, 324, 708,
        516, 109, 44, 173, 768, 660, 440, 436, 152, 772, 653, 717, 528, 108, 36, 172, 360, 504, 500, 649, 713, 781, 716,
        352, 100, 356, 1088, 641, 705, 777, 645, 709, 1152, 780, 712, 664, 769, 1216, 661, 657, 773, 665, 776,
    ),
    "inner": (
        865, 8, 872, 4, 873, 13, 309, 181, 72, 305, 177, 869, 12, 285, 68, 157, 877, 5, 277, 149, 372, 77, 9, 368, 240,
        269, 141, 76, 868, 313, 0, 185, 69, 284, 348, 244, 412, 73, 265, 137, 1, 332, 204, 317, 376, 189, 248, 64, 44,
        273, 145, 476, 604, 276, 340, 404, 540, 328, 200, 65, 32, 257, 129, 380, 252, 108, 336, 208, 261, 133, 468, 669,
        605, 293, 165, 96, 320, 192, 652, 716, 524, 324, 196, 297, 169, 356, 228, 648, 712, 520, 596, 780, 653, 717,
        589, 289, 161, 360, 281, 153, 232, 776, 649, 713, 640, 512, 585, 704, 352, 781, 644, 516, 224, 708, 301, 173,
        777, 641, 577, 280, 344, 408, 532, 768, 656, 645, 709, 581, 528, 772, 705, 300, 364, 472, 1088, 600, 536, 661,
        597, 657, 773, 1152, 593, 769, 665, 601, 1216,
    ),
}
LONG_PLAN = {
    "share": 0.359375,
    "split": 1,
    "middle": ((0, 1, 0), (0, 1, 2), (0, 1, 3), (1, 0, 0), (1, 0, 2)),
    "via": {},
    "end": (
        157, 4, 185, 0, 177, 8, 156, 68, 1, 189, 64, 149, 12, 181, 72, 9, 153, 65, 5, 129, 76, 13, 152, 73, 376, 440,
        137, 45, 368, 69, 133, 432, 77, 37, 668, 141, 504, 380, 444, 144, 109, 32, 340, 496, 145, 372, 436, 101, 33,
        165, 508, 669, 40, 173, 96, 500, 320, 36, 512, 97, 328, 712, 520, 104, 41, 324, 516, 100, 44, 332, 524, 776,
        665, 404, 161, 105, 664, 716, 169, 108, 356, 708, 160, 468, 364, 1088, 704, 532, 780, 641, 705, 168, 772, 649,
        713, 768, 645, 709, 769, 653, 717, 777, 656, 1152, 773, 657, 781, 1216, 661,
    ),
    "inner": (
        5, 0, 4, 285, 157, 69, 1, 313, 185, 64, 8, 305, 177, 68, 284, 348, 412, 376, 248, 317, 189, 65, 13, 368, 240,
        277, 149, 72, 12, 309, 181, 476, 604, 9, 380, 281, 153, 252, 77, 540, 340, 45, 212, 257, 129, 372, 76, 244, 280,
        33, 344, 73, 265, 137, 408, 669, 605, 109, 37, 261, 133, 320, 192, 97, 32, 269, 141, 328, 200, 472, 536, 272,
        36, 324, 196, 101, 273, 145, 44, 332, 204, 96, 293, 165, 40, 665, 601, 100, 301, 173, 41, 600, 336, 108, 640,
        512, 400, 356, 228, 104, 648, 520, 704, 364, 236, 105, 644, 516, 708, 641, 577, 464, 652, 524, 705, 649, 585,
        768, 289, 161, 713, 645, 581, 772, 297, 169, 709, 653, 589, 769, 528, 288, 717, 592, 352, 777, 660, 532, 716,
        773, 296, 360, 1088, 712, 657, 593, 781, 661, 597, 1152, 780, 776, 1216,
    ),
}


def decode(step):
    step, side = divmod(step, 2)
    step, part = divmod(step, 2)
    step, k = divmod(step, PAIRS)
    step, cls = divmod(step, 2)
    op, field = divmod(step, 2)
    return op, field, cls, k, part, side


def load_groups(n):
    return [[i] for i in range(3)] + [list(range(i, min(i + 8, n))) for i in range(3, n, 8)]


def when(cond, do):
    if isinstance(cond, bool):
        if cond:
            do()
    else:
        pl.when(cond)(do)


def kernel(members, blocks, wide, plan, prior_hbm, post_hbm, control_hbm, relax_hbm, ocean_hbm, out,
           x, control, ocean, relax_ref, weights, total, y_in, v_in, v_sum, a_sum, a_in, b_sum, b_in, b_swap, spread, part1, part2, factors,
           sent_bytes, load_sem, control_sem, ocean_sem, relax_sem, sent, y_recv, v_recv, a_recv, b_recv, c_recv, w_recv,
           ga_recv, gb_recv, gy_recv, gv_recv, h_recv, m_recv):
    levels, columns = control.shape
    nblocks = levels // SUB
    pairs = nblocks // 2
    rest = columns - 2 * wide
    part_width = rest // plan["split"]
    half = part_width // 2
    depth = members // 2
    m = lax.axis_index("mem")
    hz = lax.axis_index("hz")
    z = lax.div(m, 2)
    y = lax.rem(m, 2)
    other = 1 - y
    upper = z >= depth // 2
    up = jnp.where(upper, 1, 0)
    inward = jnp.where(upper, z - 1, z + 1)
    outward = jnp.where(upper, z + 1, z - 1)
    distance = jnp.where(upper, depth - 1 - z, z)
    center = depth // 2 - 1
    to_in, to_out = up, 1 - up

    def device(zz, yy):
        return {"mem": zz * 2 + yy, "hz": hz}

    barrier = pltpu.get_barrier_semaphore()

    def greet(to):
        pl.semaphore_signal(barrier, inc=1, device_id=to, device_id_type=MESH)

    greet(device(z, other))
    greet(device(inward, y))
    pl.when(distance > 0)(lambda: greet(device(outward, y)))
    for i in range(1, blocks):
        greet({"mem": m, "hz": lax.rem(hz + i, blocks)})

    def block_of(k, side):
        return k + pairs * (up if side == NEAR else 1 - up)

    def rows(block):
        return pl.ds(pl.multiple_of(block * SUB, SUB), SUB)

    def wide_cols(yy):
        return pl.ds(pl.multiple_of(yy * wide, LANE), wide)

    def rest_cols(part):
        return pl.ds(2 * wide + part * part_width, part_width)

    fields = (post_hbm, prior_hbm)

    via_index = {chunk: i for i, chunk in enumerate(sorted(plan["via"]))}
    middle_index = {chunk: i for i, chunk in enumerate(plan["middle"])}

    ocean_load = pltpu.make_async_copy(ocean_hbm, ocean, ocean_sem)
    ocean_load.start()
    first_use = []
    for step in plan["end"]:
        op, field, cls, k, part, side = decode(step)
        if op < STAT1 and (field, k, side) not in first_use:
            first_use.append((field, k, side))
    groups = load_groups(len(first_use))
    group_of = {}
    for i, group in enumerate(groups):
        for n in group:
            field, k, side = first_use[n]
            block = block_of(k, side)
            group_of[first_use[n]] = i
            pltpu.make_async_copy(fields[field].at[0, rows(block)], x.at[field, rows(block)], load_sem.at[i]).start()
    control_load = pltpu.make_async_copy(control_hbm, control, control_sem)
    control_load.start()
    relax_load = pltpu.make_async_copy(relax_hbm, relax_ref, relax_sem)
    relax_load.start()
    pl.semaphore_wait(barrier, 1 + blocks + jnp.where(distance > 0, 1, 0))

    def arrive(dst, recv_sem):
        pltpu.make_async_remote_copy(src_ref=dst, dst_ref=dst, send_sem=sent, recv_sem=recv_sem,
                                     device_id=device(z, other), device_id_type=MESH).wait_recv()

    def merge(own, n_own, came, n_came, w, dst, field, block, scale=1.0):
        acc = jnp.zeros((SUB, LANE), jnp.float32)
        static = isinstance(n_own, int) and isinstance(n_came, int)
        equal = static and n_own == n_came
        if not static:
            f_own, f_came = (jnp.float32(n) if isinstance(n, int) else n.astype(jnp.float32) for n in (n_own, n_came))
        for j in range(own.shape[-1] // LANE):
            at = slice(j * LANE, (j + 1) * LANE)
            a, b = own[:, at], came[:, at]
            if equal:
                d = b - a
            elif static:
                d = b * float(n_own) - a * float(n_came)
            else:
                d = b * f_own - a * f_came
            acc += d * d * w[:, at]
            if dst is not None:
                dst[:, at] = a + b
        if equal:
            acc = acc * (scale / (2 * n_own))
        elif static:
            acc = acc * (scale / (n_own * n_came * (n_own + n_came)))
        else:
            acc = acc / jnp.full((SUB, LANE), f_own * f_came * (f_own + f_came), jnp.float32) * scale
        spread[field, block] += acc

    lane = lax.broadcasted_iota(jnp.int32, (SUB, LANE), 1)
    sub = lax.broadcasted_iota(jnp.int32, (SUB, LANE), 0)

    def role(order, end):
        pending = []
        loaded = set()
        finished = []
        state = {"factor": False, "weights": False}
        far = 0 if end else (1 if center == 1 else distance)
        at_center = False if end else (True if center == 1 else distance == center)
        before = False if end else (False if center == 1 else distance < center)
        last_step = {}
        for i, step in enumerate(order):
            op, *chunk = decode(step)
            if op in (AG_OUT, AGY_SEND):
                last_step[tuple(chunk)] = i

        def prepare():
            state["weights"] = True
            ocean_load.wait()
            weights[...] = jnp.broadcast_to(ocean[...].astype(jnp.float32), (SUB, columns))
            spread[...] = jnp.zeros_like(spread)

        def via(field, k, side):
            v = plan["via"].get((field, k, side), 0)
            return 0 if v == 0 else (1 if (v == 1) == end else 2)

        def own_count(field, k, side, here=True):
            v = via(field, k, side)
            return (2, 3, 1)[v] if here else (2, 1, 3)[v]

        def send(src, dst, recv_sem, to, cond=True):
            copy = pltpu.make_async_remote_copy(src_ref=src, dst_ref=dst, send_sem=sent, recv_sem=recv_sem,
                                                device_id=to, device_id_type=MESH)
            when(cond, copy.start)
            pending.append((cond, copy, src.size if hasattr(src, "size") else math.prod(src.shape)))

        def local(field, k, side):
            block = block_of(k, side)
            group = group_of[field, k, side]
            if group not in loaded:
                loaded.add(group)
                some = x.at[field, pl.ds(0, len(groups[group]) * SUB)]
                pltpu.make_async_copy(fields[field].at[0, pl.ds(0, len(groups[group]) * SUB)], some, load_sem.at[group]).wait()
            return block

        def chain_sem(field, cls, k, part, side, direction):
            if side == NEAR and direction is to_in and (field, cls, k) in middle_index:
                return c_recv.at[middle_index[field, cls, k], part]
            block = block_of(k, side)
            return a_recv.at[field, block] if cls == ROWS_FIRST else b_recv.at[field, block, part]

        def raw(field, block, cols):
            return x.at[field, rows(block), cols]

        def chain_send(field, cls, k, part, side, direction, to, cond=True):
            block = local(field, k, side)
            first = end and (side == FAR or (field, cls, k) in plan["middle"])
            if cls == ROWS_FIRST:
                src = raw(field, block, wide_cols(y)) if first and via(field, k, side) == 2 else a_sum.at[field, block]
                at, came = (field, block, direction), a_in
            else:
                src = raw(field, block, rest_cols(part)) if first else b_sum.at[field, block, part]
                at, came = (field, block, direction, part), b_in
            send(src, came.at[at], chain_sem(field, cls, k, part, side, direction), to, cond)

        def chain_merge(field, cls, k, part, side, direction, n_own, n_came, first, total_too=False):
            block = local(field, k, side)
            if cls == ROWS_FIRST:
                at = (field, block, direction)
                own = raw(field, block, wide_cols(y)) if first and via(field, k, side) == 2 else a_sum.at[field, block]
                into = a_sum.at[field, block]
                if total_too:
                    into = spot(cls, block, part) if field == POST else None
                arrive(a_in.at[at], chain_sem(field, cls, k, part, side, direction))
                merge(own, n_own, a_in.at[at], n_came, weights.at[:, wide_cols(y)], into, field, block)
            else:
                at = (field, block, direction, part)
                own = raw(field, block, rest_cols(part)) if first else b_sum.at[field, block, part]
                arrive(b_in.at[at], chain_sem(field, cls, k, part, side, direction))
                merge(own, n_own, b_in.at[at], n_came, weights.at[:, rest_cols(part)], b_sum.at[field, block, part], field, block)

        def spot(cls, block, part):
            return total.at[rows(block), wide_cols(y) if cls == ROWS_FIRST else rest_cols(part)]

        def total_sem(cls, block, part):
            return ga_recv.at[block] if cls == ROWS_FIRST else gb_recv.at[block, part]

        def total_send(cls, block, part, to, cond=True):
            send(spot(cls, block, part), spot(cls, block, part), total_sem(cls, block, part), to, cond)

        def total_arrive(cls, block, part):
            arrive(spot(cls, block, part), total_sem(cls, block, part))

        def half_send(block, yy, sem, to, cond=True):
            at = total.at[rows(block), wide_cols(yy)]
            send(at, at, sem, to, cond)

        def finish(block, cols):
            f = factors[block]
            c, p, t, o = (r.at[rows(block), cols] for r in (control, x.at[POST], total, out.at[0]))
            for j in range(c.shape[-1] // LANE):
                at = slice(j * LANE, (j + 1) * LANE)
                o[:, at] = c[:, at] + f * (p[:, at] - t[:, at] * (1.0 / members))

        def ready(block, cols):
            if state["factor"]:
                finish(block, cols)
            else:
                finished.append((block, cols))

        def do_step(i, step):
            op, field, cls, k, part, side = decode(step)
            if not state["weights"] and op in (Y_RECV, V_RECV, RS_FROM_OUT, RS_FROM_IN):
                prepare()
            if op < STAT1:
                middle = (field, cls, k) in plan["middle"]
                block = block_of(k, side)
                root_here = side == NEAR and end != middle
                here = True if end or not root_here else at_center
                rows_first = cls == ROWS_FIRST
                cols = wide_cols(y) if rows_first else rest_cols(part)
                v = via(field, k, side) if rows_first else 0
                chunk = (field, cls, k, part, side)
                if rows_first:
                    own, came = own_count(field, k, side), own_count(field, k, side, False)
                    out_count = 2 * far if v == 0 else came
                    end_count = 2 * (depth - 1) if v == 0 else 2 * depth - own
                    in_count, near_count = 2 * (depth - 1 - far), 2 * (far + 1)
                else:
                    own, out_count, end_count, in_count, near_count = 1, far, depth - 1, depth - 1 - far, far + 1
            if op == Y_SEND:
                local(field, k, side)
                src = v_sum.at[field, block] if v == 1 else raw(field, block, wide_cols(other))
                send(src, y_in.at[field, block], y_recv.at[field, block], device(z, other))
            elif op == Y_RECV:
                local(field, k, side)
                arrive(y_in.at[field, block], y_recv.at[field, block])
                merge(raw(field, block, wide_cols(y)), 1, y_in.at[field, block], 2 if v == 1 else 1, weights.at[:, wide_cols(y)],
                      a_sum.at[field, block], field, block)
            elif op == V_SEND:
                local(field, k, side)
                send(raw(field, block, wide_cols(other)), v_in.at[field, block], v_recv.at[via_index[field, k, side]],
                     device(inward if end else outward, y))
            elif op == V_RECV:
                local(field, k, side)
                arrive(v_in.at[field, block], v_recv.at[via_index[field, k, side]])
                merge(raw(field, block, wide_cols(other)), 1, v_in.at[field, block], 1, weights.at[:, wide_cols(other)],
                      v_sum.at[field, block], field, block)
            elif op == RS_IN:
                chain_send(*chunk, to_in, device(inward, y))
            elif op == RS_OUT:
                chain_send(*chunk, to_out, device(outward, y))
            elif op == RS_FROM_OUT:
                chain_merge(*chunk, to_in, own, out_count, True)
                if root_here and before is not False:
                    chain_send(*chunk, to_in, device(inward, y), before)
            elif op == RS_FROM_IN:
                if end:
                    chain_merge(*chunk, to_out, own, end_count, True, True)
                elif not middle:
                    chain_merge(*chunk, to_out, own, in_count, True)
                else:
                    when(here, lambda: chain_merge(*chunk, to_out, near_count, in_count, False, True))
                if rows_first and field == POST and root_here and before is False:
                    ready(block, cols)
            elif op == SW_SEND:
                at = (field, block, part)
                if field == POST:
                    send(b_sum.at[at], b_swap.at[at], w_recv.at[field, k, part], device(z, other), here)
                else:
                    send(b_sum.at[(*at, slice(None), pl.ds(pl.multiple_of(other * half, LANE), half))],
                         b_swap.at[(*at, slice(None), pl.ds(0, half))], w_recv.at[field, k, part], device(z, other), here)
            elif op == SW_RECV:
                at = (field, block, part)

                def swap():
                    if field == POST:
                        arrive(b_swap.at[at], w_recv.at[field, k, part])
                        merge(b_sum.at[at], depth, b_swap.at[at], depth, weights.at[:, rest_cols(part)], spot(cls, block, part),
                              field, block, 0.5)
                    else:
                        came = b_swap.at[(*at, slice(None), pl.ds(0, half))]
                        arrive(came, w_recv.at[field, k, part])
                        mine = pl.ds(pl.multiple_of(y * half, LANE), half)
                        place = pl.ds(pl.multiple_of(2 * wide + part * part_width + y * half, LANE), half)
                        merge(b_sum.at[(*at, slice(None), mine)], depth, came, depth, weights.at[:, place], None, field, block)

                when(here, swap)
                if field == POST and before is False:
                    ready(block, cols)
            elif op == AG_IN:
                total_send(cls, block, part, device(inward, y), here)
            elif op in (AG_OUT, AGY_SEND):
                if op == AG_OUT:
                    total_send(cls, block, part, device(outward, y), here)
                else:
                    half_send(block, y, gy_recv.at[block], device(z, other), here)
                if root_here and before is not False and last_step[chunk] == i:
                    when(before, lambda: total_arrive(cls, block, part))
                    total_send(cls, block, part, device(outward, y), before)
                    if rows_first:
                        half_send(block, y, gy_recv.at[block], device(z, other), before)
                    ready(block, cols)
            elif op == AG_RECV:
                total_arrive(cls, block, part)
                ready(block, cols)
            elif op in (AGY_RECV, W_RECV):
                sem = gy_recv.at[block] if op == AGY_RECV else gv_recv.at[via_index[field, k, side]]
                arrive(total.at[rows(block), wide_cols(other)], sem)
                ready(block, wide_cols(other))
            elif op == W_SEND:
                half_send(block, other, gv_recv.at[via_index[field, k, side]], device(inward if end else outward, y))
            elif op == STAT1:
                for field in (POST, PRIOR):
                    packed = jnp.zeros((SUB, LANE), jnp.float32)
                    for b in range(nblocks):
                        packed = jnp.where(lane == b, jnp.sum(spread[field, b], axis=1, keepdims=True), packed)
                    part1[hz, field] = packed
                for b in range(1, blocks):
                    send(part1.at[hz], part1.at[hz], h_recv, {"mem": m, "hz": lax.rem(hz + b, blocks)})
            elif op == STAT2:
                arrive(part1.at[pl.ds(0, blocks - 1)], h_recv)
                for field in (POST, PRIOR):
                    v = part1[0, field]
                    for b in range(1, blocks):
                        v = v + part1[b, field]
                    part2[m, field] = v
                for b in range(1, members):
                    send(part2.at[m], part2.at[m], m_recv, {"mem": lax.rem(m + b, members), "hz": hz})
            elif op == STAT3:
                arrive(part2.at[pl.ds(0, members - 1)], m_recv)
                sums = []
                for field in (POST, PRIOR):
                    v = part2[0, field]
                    for b in range(1, members):
                        v = v + part2[b, field]
                    sums.append(v)
                relax_load.wait()
                relax = jnp.zeros((SUB, LANE), jnp.float32)
                for level in range(levels):
                    relax = jnp.where((sub == level % SUB) & (lane == level // SUB), relax_ref[level], relax)
                factor = relax * (jnp.sqrt((sums[PRIOR] + eps) / (sums[POST] + eps)) - 1.0) + 1.0
                for b in range(nblocks):
                    factors[b] = jnp.broadcast_to(
                        jnp.sum(jnp.where(lane == b, factor, 0.0), axis=1, keepdims=True), (SUB, LANE))
                control_load.wait()
                state["factor"] = True
            if state["factor"] and finished:
                for _ in range(2):
                    if finished:
                        finish(*finished.pop(0))
        for i, step in enumerate(order):
            do_step(i, step)
        for todo in finished:
            finish(*todo)
        if all(isinstance(cond, bool) for cond, _, _ in pending):
            tiles = sum(size for cond, _, size in pending if cond) // (SUB * LANE)
            all_sent = sent_bytes.at[pl.ds(0, tiles * SUB)]
            pltpu.make_async_copy(all_sent, all_sent, sent).wait()
        else:
            for cond, copy, _ in pending:
                when(cond, copy.wait_send)

    @pl.when(distance == 0)
    def _():
        role(plan["end"], True)

    @pl.when(distance > 0)
    def _():
        role(plan["inner"], False)


def solution(mesh):
    members, blocks = mesh.shape["mem"], mesh.shape["hz"]
    plan = PLAN if members // 2 == SHORT_LINE else LONG_PLAN

    def on_device(prior, posterior, control, relax, ocean):
        levels, columns = control.shape
        n = levels // SUB
        wide = round(columns * plan["share"] / LANE) * LANE
        parts = plan["split"]
        rest = (columns - 2 * wide) // parts
        vmem = lambda *shape: pltpu.VMEM(shape, jnp.float32)
        dma = lambda *shape: pltpu.SemaphoreType.DMA(shape)
        one = pltpu.SemaphoreType.DMA
        return pl.pallas_call(
            functools.partial(kernel, members, blocks, wide, plan),
            out_shape=pltpu.VMEM(posterior.shape, jnp.float32),
            in_specs=[pl.BlockSpec(memory_space=pltpu.HBM)] * 5,
            out_specs=pl.BlockSpec(memory_space=pltpu.VMEM),
            scratch_shapes=[
                vmem(2, levels, columns), vmem(levels, columns), pltpu.VMEM((1, columns), jnp.int32),
                pltpu.SMEM((levels,), jnp.float32), vmem(SUB, columns), vmem(levels, columns),
                vmem(2, n, SUB, wide), vmem(2, n, SUB, wide), vmem(2, n, SUB, wide), vmem(2, n, SUB, wide),
                vmem(2, n, 2, SUB, wide), vmem(2, n, parts, SUB, rest), vmem(2, n, 2, parts, SUB, rest),
                vmem(2, n, parts, SUB, rest), vmem(2, n, SUB, LANE), vmem(blocks, 2, SUB, LANE),
                vmem(members, 2, SUB, LANE), vmem(n, SUB, LANE),
                vmem(4 * levels * columns // LANE, LANE),
                dma(len(load_groups(2 * n))), one, one, one, one, dma(2, n), dma(max(1, len(plan["via"]))), dma(2, n),
                dma(2, n, parts), dma(max(1, len(plan["middle"])), parts), dma(2, n // 2, parts),
                dma(n), dma(n, parts), dma(n), dma(max(1, len(plan["via"]))), one, one,
            ],
            compiler_params=pltpu.CompilerParams(
                collective_id=0, has_side_effects=True, vmem_limit_bytes=60 * 2**20
            ),
        )(prior, posterior, control, relax, ocean.reshape(1, columns))

    return jax.shard_map(
        on_device,
        mesh=mesh,
        in_specs=(P("mem", None, "hz"), P("mem", None, "hz"), P(None, "hz"), P(), P("hz")),
        out_specs=P("mem", None, "hz"),
        check_vma=False,
    )
```

```python
import functools
import math

import jax
import jax.numpy as jnp
from jax import lax
from jax.experimental import pallas as pl
from jax.experimental.pallas import tpu as pltpu
from jax.sharding import PartitionSpec as P

eps = 1e-06
SUB = 8
LANE = 128
MESH = pl.DeviceIdType.MESH
POST, PRIOR = 0, 1
ROWS_FIRST, DEPTH_FIRST = 0, 1
NEAR, FAR = 0, 1
PAIRS = 4
SHORT_LINE = 4

(Y_SEND, Y_RECV, RS_IN, RS_OUT, RS_FROM_OUT, RS_FROM_IN, SW_SEND, SW_RECV, AG_IN, AG_OUT, AG_RECV,
 AGY_SEND, AGY_RECV, V_SEND, V_RECV, W_SEND, W_RECV, STAT1, STAT2, STAT3) = range(20)

PLAN = {
    "share": 0.390625,
    "split": 1,
    "middle": ((0, 0, 0), (0, 1, 0), (1, 0, 3)),
    "via": {(0, 1, 0): 2, (1, 0, 1): 1, (1, 1, 0): 1, (1, 1, 1): 1, (1, 2, 1): 1, (1, 3, 1): 1},
    "end": (
        189, 1, 145, 8, 157, 149, 9, 181, 65, 937, 144, 13, 153, 72, 941, 177, 12, 73, 933, 137, 37, 77, 932, 141, 5,
        129, 76, 929, 0, 348, 836, 101, 340, 41, 372, 69, 133, 380, 436, 40, 656, 64, 128, 368, 36, 344, 105, 169, 500,
        33, 185, 328, 104, 520, 712, 657, 100, 165, 44, 332, 97, 161, 45, 640, 776, 524, 432, 408, 324, 108, 516, 404,
        444, 641, 109, 412, 173, 496, 704, 472, 360, 536, 468, 376, 440, 508, 532, 32, 476, 540, 649, 172, 713, 768,
        504, 356, 716, 96, 352, 1088, 705, 777, 653, 717, 780, 645, 1152, 709, 769, 1028, 665, 1216, 781, 661, 669, 773,
    ),
    "inner": (
        873, 9, 877, 8, 869, 13, 317, 189, 73, 273, 145, 868, 44, 285, 157, 72, 277, 149, 865, 1, 380, 309, 181, 77,
        272, 336, 400, 348, 220, 281, 153, 32, 108, 340, 212, 305, 177, 372, 244, 5, 65, 252, 265, 137, 464, 592, 344,
        0, 528, 368, 240, 269, 96, 216, 141, 12, 257, 69, 129, 328, 200, 40, 657, 900, 64, 593, 4, 261, 133, 76, 332,
        204, 256, 320, 704, 512, 576, 104, 297, 169, 68, 324, 196, 313, 185, 768, 641, 705, 577, 648, 520, 712, 360,
        232, 293, 165, 376, 248, 289, 161, 769, 649, 713, 585, 652, 524, 716, 776, 356, 228, 644, 516, 708, 352, 224,
        777, 301, 173, 653, 717, 589, 664, 780, 536, 660, 532, 645, 709, 581, 668, 772, 540, 964, 300, 364, 1088, 781,
        665, 601, 661, 597, 773, 669, 1152, 605, 1216,
    ),
}
LONG_PLAN = {
    "share": 0.359375,
    "split": 1,
    "middle": ((0, 1, 0), (0, 1, 2), (0, 1, 3), (1, 0, 0), (1, 0, 2)),
    "via": {},
    "end": (
        157, 4, 185, 0, 177, 8, 156, 68, 1, 189, 64, 149, 12, 181, 72, 9, 153, 65, 5, 129, 76, 13, 152, 73, 376, 440,
        137, 45, 368, 69, 133, 432, 77, 37, 668, 141, 504, 380, 444, 144, 109, 32, 340, 496, 145, 372, 436, 101, 33,
        165, 508, 669, 40, 173, 96, 500, 320, 36, 512, 97, 328, 712, 520, 104, 41, 324, 516, 100, 44, 332, 524, 776,
        665, 404, 161, 105, 664, 716, 169, 108, 356, 708, 160, 468, 364, 1088, 704, 532, 780, 641, 705, 168, 772, 649,
        713, 768, 645, 709, 769, 653, 717, 777, 656, 1152, 773, 657, 781, 1216, 661,
    ),
    "inner": (
        5, 0, 4, 285, 157, 69, 1, 313, 185, 64, 8, 305, 177, 68, 284, 348, 412, 376, 248, 317, 189, 65, 13, 368, 240,
        277, 149, 72, 12, 309, 181, 476, 604, 9, 380, 281, 153, 252, 77, 540, 340, 45, 212, 257, 129, 372, 76, 244, 280,
        33, 344, 73, 265, 137, 408, 669, 605, 109, 37, 261, 133, 320, 192, 97, 32, 269, 141, 328, 200, 472, 536, 272,
        36, 324, 196, 101, 273, 145, 44, 332, 204, 96, 293, 165, 40, 665, 601, 100, 301, 173, 41, 600, 336, 108, 640,
        512, 400, 356, 228, 104, 648, 520, 704, 364, 236, 105, 644, 516, 708, 641, 577, 464, 652, 524, 705, 649, 585,
        768, 289, 161, 713, 645, 581, 772, 297, 169, 709, 653, 589, 769, 528, 288, 717, 592, 352, 777, 660, 532, 716,
        773, 296, 360, 1088, 712, 657, 593, 781, 661, 597, 1152, 780, 776, 1216,
    ),
}


def decode(step):
    step, side = divmod(step, 2)
    step, part = divmod(step, 2)
    step, k = divmod(step, PAIRS)
    step, cls = divmod(step, 2)
    op, field = divmod(step, 2)
    return op, field, cls, k, part, side


def load_groups(n):
    return [[i] for i in range(3)] + [list(range(i, min(i + 8, n))) for i in range(3, n, 8)]


def when(cond, do):
    if isinstance(cond, bool):
        if cond:
            do()
    else:
        pl.when(cond)(do)


def kernel(members, blocks, wide, plan, prior_hbm, post_hbm, control_hbm, relax_hbm, ocean_hbm, out,
           x, control, ocean, relax_ref, weights, total, y_in, v_in, v_sum, a_sum, a_in, b_sum, b_in, b_swap, spread, part1, part2, factors,
           sent_bytes, load_sem, control_sem, ocean_sem, relax_sem, sent, y_recv, v_recv, a_recv, b_recv, c_recv, w_recv,
           gy_recv, h_recv, m_recv):
    levels, columns = control.shape
    nblocks = levels // SUB
    pairs = nblocks // 2
    rest = columns - 2 * wide
    part_width = rest // plan["split"]
    half = part_width // 2
    depth = members // 2
    m = lax.axis_index("mem")
    hz = lax.axis_index("hz")
    z = lax.div(m, 2)
    y = lax.rem(m, 2)
    other = 1 - y
    upper = z >= depth // 2
    up = jnp.where(upper, 1, 0)
    inward = jnp.where(upper, z - 1, z + 1)
    outward = jnp.where(upper, z + 1, z - 1)
    distance = jnp.where(upper, depth - 1 - z, z)
    center = depth // 2 - 1
    to_in, to_out = up, 1 - up

    def device(zz, yy):
        return {"mem": zz * 2 + yy, "hz": hz}

    barrier = pltpu.get_barrier_semaphore()

    def greet(to):
        pl.semaphore_signal(barrier, inc=1, device_id=to, device_id_type=MESH)

    greet(device(z, other))
    greet(device(inward, y))
    pl.when(distance > 0)(lambda: greet(device(outward, y)))
    for i in range(1, blocks):
        greet({"mem": m, "hz": lax.rem(hz + i, blocks)})

    def block_of(k, side):
        return k + pairs * (up if side == NEAR else 1 - up)

    def rows(block):
        return pl.ds(pl.multiple_of(block * SUB, SUB), SUB)

    def wide_cols(yy):
        return pl.ds(pl.multiple_of(yy * wide, LANE), wide)

    def rest_cols(part):
        return pl.ds(2 * wide + part * part_width, part_width)

    fields = (post_hbm, prior_hbm)

    via_index = {chunk: i for i, chunk in enumerate(sorted(plan["via"]))}
    middle_index = {chunk: i for i, chunk in enumerate(plan["middle"])}

    ocean_load = pltpu.make_async_copy(ocean_hbm, ocean, ocean_sem)
    ocean_load.start()
    first_use = []
    for step in plan["end"]:
        op, field, cls, k, part, side = decode(step)
        if op < STAT1 and (field, k, side) not in first_use:
            first_use.append((field, k, side))
    groups = load_groups(len(first_use))
    group_of = {}
    for i, group in enumerate(groups):
        for n in group:
            field, k, side = first_use[n]
            block = block_of(k, side)
            group_of[first_use[n]] = i
            pltpu.make_async_copy(fields[field].at[0, rows(block)], x.at[field, rows(block)], load_sem.at[i]).start()
    control_load = pltpu.make_async_copy(control_hbm, control, control_sem)
    control_load.start()
    relax_load = pltpu.make_async_copy(relax_hbm, relax_ref, relax_sem)
    relax_load.start()
    pl.semaphore_wait(barrier, 1 + blocks + jnp.where(distance > 0, 1, 0))

    def arrive(dst, recv_sem):
        pltpu.make_async_remote_copy(src_ref=dst, dst_ref=dst, send_sem=sent, recv_sem=recv_sem,
                                     device_id=device(z, other), device_id_type=MESH).wait_recv()

    def merge(own, n_own, came, n_came, w, dst, field, block, scale=1.0):
        acc = jnp.zeros((SUB, LANE), jnp.float32)
        static = isinstance(n_own, int) and isinstance(n_came, int)
        equal = static and n_own == n_came
        if not static:
            f_own, f_came = (jnp.float32(n) if isinstance(n, int) else n.astype(jnp.float32) for n in (n_own, n_came))
        for j in range(own.shape[-1] // LANE):
            at = slice(j * LANE, (j + 1) * LANE)
            a, b = own[:, at], came[:, at]
            if equal:
                d = b - a
            elif static:
                d = b * float(n_own) - a * float(n_came)
            else:
                d = b * f_own - a * f_came
            acc += d * d * w[:, at]
            if dst is not None:
                dst[:, at] = a + b
        if equal:
            acc = acc * (scale / (2 * n_own))
        elif static:
            acc = acc * (scale / (n_own * n_came * (n_own + n_came)))
        else:
            acc = acc / jnp.full((SUB, LANE), f_own * f_came * (f_own + f_came), jnp.float32) * scale
        spread[field, block] += acc

    lane = lax.broadcasted_iota(jnp.int32, (SUB, LANE), 1)
    sub = lax.broadcasted_iota(jnp.int32, (SUB, LANE), 0)

    def role(order, end):
        pending = []
        loaded = set()
        finished = []
        state = {"factor": False, "weights": False}
        far = 0 if end else (1 if center == 1 else distance)
        at_center = False if end else (True if center == 1 else distance == center)
        before = False if end else (False if center == 1 else distance < center)
        last_step = {}
        for i, step in enumerate(order):
            op, *chunk = decode(step)
            if op in (AG_OUT, AGY_SEND):
                last_step[tuple(chunk)] = i

        def prepare():
            state["weights"] = True
            ocean_load.wait()
            weights[...] = jnp.broadcast_to(ocean[...].astype(jnp.float32), (SUB, columns))
            spread[...] = jnp.zeros_like(spread)

        def via(field, k, side):
            v = plan["via"].get((field, k, side), 0)
            return 0 if v == 0 else (1 if (v == 1) == end else 2)

        def own_count(field, k, side, here=True):
            v = via(field, k, side)
            return (2, 3, 1)[v] if here else (2, 1, 3)[v]

        def send(src, dst, recv_sem, to, cond=True):
            copy = pltpu.make_async_remote_copy(src_ref=src, dst_ref=dst, send_sem=sent, recv_sem=recv_sem,
                                                device_id=to, device_id_type=MESH)
            when(cond, copy.start)
            pending.append((cond, copy, src.size if hasattr(src, "size") else math.prod(src.shape)))

        def local(field, k, side):
            block = block_of(k, side)
            group = group_of[field, k, side]
            if group not in loaded:
                loaded.add(group)
                some = x.at[field, pl.ds(0, len(groups[group]) * SUB)]
                pltpu.make_async_copy(fields[field].at[0, pl.ds(0, len(groups[group]) * SUB)], some, load_sem.at[group]).wait()
            return block

        def chain_sem(field, cls, k, part, side, direction):
            if side == NEAR and direction is to_in and (field, cls, k) in middle_index:
                return c_recv.at[middle_index[field, cls, k], part]
            block = block_of(k, side)
            return a_recv.at[field, block] if cls == ROWS_FIRST else b_recv.at[field, block, part]

        def raw(field, block, cols):
            return x.at[field, rows(block), cols]

        def chain_send(field, cls, k, part, side, direction, to, cond=True):
            block = local(field, k, side)
            first = end and (side == FAR or (field, cls, k) in plan["middle"])
            if cls == ROWS_FIRST:
                src = raw(field, block, wide_cols(y)) if first and via(field, k, side) == 2 else a_sum.at[field, block]
                at, came = (field, block, direction), a_in
            else:
                src = raw(field, block, rest_cols(part)) if first else b_sum.at[field, block, part]
                at, came = (field, block, direction, part), b_in
            send(src, came.at[at], chain_sem(field, cls, k, part, side, direction), to, cond)

        def chain_merge(field, cls, k, part, side, direction, n_own, n_came, first, total_too=False):
            block = local(field, k, side)
            if cls == ROWS_FIRST:
                at = (field, block, direction)
                own = raw(field, block, wide_cols(y)) if first and via(field, k, side) == 2 else a_sum.at[field, block]
                into = a_sum.at[field, block]
                if total_too:
                    into = spot(cls, block, part) if field == POST else None
                arrive(a_in.at[at], chain_sem(field, cls, k, part, side, direction))
                merge(own, n_own, a_in.at[at], n_came, weights.at[:, wide_cols(y)], into, field, block)
            else:
                at = (field, block, direction, part)
                own = raw(field, block, rest_cols(part)) if first else b_sum.at[field, block, part]
                arrive(b_in.at[at], chain_sem(field, cls, k, part, side, direction))
                merge(own, n_own, b_in.at[at], n_came, weights.at[:, rest_cols(part)], b_sum.at[field, block, part], field, block)

        def spot(cls, block, part):
            return total.at[rows(block), wide_cols(y) if cls == ROWS_FIRST else rest_cols(part)]

        def total_sem(cls, block, part):
            return a_recv.at[POST, block] if cls == ROWS_FIRST else b_recv.at[POST, block, part]

        def total_send(cls, block, part, to, cond=True):
            send(spot(cls, block, part), spot(cls, block, part), total_sem(cls, block, part), to, cond)

        def total_arrive(cls, block, part):
            arrive(spot(cls, block, part), total_sem(cls, block, part))

        def half_send(block, yy, sem, to, cond=True):
            at = total.at[rows(block), wide_cols(yy)]
            send(at, at, sem, to, cond)

        def tiles(width):
            for j in range(0, width // LANE, 8):
                yield [slice(i * LANE, (i + 1) * LANE) for i in range(j, min(j + 8, width // LANE))]

        def anomaly(block, cols):
            p, t, o = (r.at[rows(block), cols] for r in (x.at[POST], total, out.at[0]))
            for some in tiles(o.shape[-1]):
                for at, v in [(at, p[:, at] - t[:, at] * (1.0 / members)) for at in some]:
                    o[:, at] = v

        def finish(block, cols):
            f = factors[block]
            c, o = control.at[rows(block), cols], out.at[0, rows(block), cols]
            for some in tiles(o.shape[-1]):
                for at, v in [(at, c[:, at] + f * o[:, at]) for at in some]:
                    o[:, at] = v

        def ready(block, cols):
            anomaly(block, cols)
            if state["factor"]:
                finish(block, cols)
            else:
                finished.append((block, cols))

        def do_step(i, step):
            op, field, cls, k, part, side = decode(step)
            if not state["weights"] and op in (Y_RECV, V_RECV, RS_FROM_OUT, RS_FROM_IN):
                prepare()
            if op < STAT1:
                middle = (field, cls, k) in plan["middle"]
                block = block_of(k, side)
                root_here = side == NEAR and end != middle
                here = True if end or not root_here else at_center
                rows_first = cls == ROWS_FIRST
                cols = wide_cols(y) if rows_first else rest_cols(part)
                v = via(field, k, side) if rows_first else 0
                chunk = (field, cls, k, part, side)
                if rows_first:
                    own, came = own_count(field, k, side), own_count(field, k, side, False)
                    out_count = 2 * far if v == 0 else came
                    end_count = 2 * (depth - 1) if v == 0 else 2 * depth - own
                    in_count, near_count = 2 * (depth - 1 - far), 2 * (far + 1)
                else:
                    own, out_count, end_count, in_count, near_count = 1, far, depth - 1, depth - 1 - far, far + 1
            if op == Y_SEND:
                local(field, k, side)
                src = v_sum.at[field, block] if v == 1 else raw(field, block, wide_cols(other))
                send(src, y_in.at[field, block], y_recv.at[field, block], device(z, other))
            elif op == Y_RECV:
                local(field, k, side)
                arrive(y_in.at[field, block], y_recv.at[field, block])
                merge(raw(field, block, wide_cols(y)), 1, y_in.at[field, block], 2 if v == 1 else 1, weights.at[:, wide_cols(y)],
                      a_sum.at[field, block], field, block)
            elif op == V_SEND:
                local(field, k, side)
                send(raw(field, block, wide_cols(other)), v_in.at[field, block], v_recv.at[via_index[field, k, side]],
                     device(inward if end else outward, y))
            elif op == V_RECV:
                local(field, k, side)
                arrive(v_in.at[field, block], v_recv.at[via_index[field, k, side]])
                merge(raw(field, block, wide_cols(other)), 1, v_in.at[field, block], 1, weights.at[:, wide_cols(other)],
                      v_sum.at[field, block], field, block)
            elif op == RS_IN:
                chain_send(*chunk, to_in, device(inward, y))
            elif op == RS_OUT:
                chain_send(*chunk, to_out, device(outward, y))
            elif op == RS_FROM_OUT:
                chain_merge(*chunk, to_in, own, out_count, True)
                if root_here and before is not False:
                    chain_send(*chunk, to_in, device(inward, y), before)
            elif op == RS_FROM_IN:
                if end:
                    chain_merge(*chunk, to_out, own, end_count, True, True)
                elif not middle:
                    chain_merge(*chunk, to_out, own, in_count, True)
                else:
                    when(here, lambda: chain_merge(*chunk, to_out, near_count, in_count, False, True))
                if rows_first and field == POST and root_here and before is False:
                    ready(block, cols)
            elif op == SW_SEND:
                at = (field, block, part)
                if field == POST:
                    send(b_sum.at[at], b_swap.at[at], w_recv.at[field, k, part], device(z, other), here)
                else:
                    send(b_sum.at[(*at, slice(None), pl.ds(pl.multiple_of(other * half, LANE), half))],
                         b_swap.at[(*at, slice(None), pl.ds(0, half))], w_recv.at[field, k, part], device(z, other), here)
            elif op == SW_RECV:
                at = (field, block, part)

                def swap():
                    if field == POST:
                        arrive(b_swap.at[at], w_recv.at[field, k, part])
                        merge(b_sum.at[at], depth, b_swap.at[at], depth, weights.at[:, rest_cols(part)], spot(cls, block, part),
                              field, block, 0.5)
                    else:
                        came = b_swap.at[(*at, slice(None), pl.ds(0, half))]
                        arrive(came, w_recv.at[field, k, part])
                        mine = pl.ds(pl.multiple_of(y * half, LANE), half)
                        place = pl.ds(pl.multiple_of(2 * wide + part * part_width + y * half, LANE), half)
                        merge(b_sum.at[(*at, slice(None), mine)], depth, came, depth, weights.at[:, place], None, field, block)

                when(here, swap)
                if field == POST and before is False:
                    ready(block, cols)
            elif op == AG_IN:
                total_send(cls, block, part, device(inward, y), here)
            elif op in (AG_OUT, AGY_SEND):
                if op == AG_OUT:
                    total_send(cls, block, part, device(outward, y), here)
                else:
                    half_send(block, y, gy_recv.at[block], device(z, other), here)
                if root_here and before is not False and last_step[chunk] == i:
                    when(before, lambda: total_arrive(cls, block, part))
                    total_send(cls, block, part, device(outward, y), before)
                    if rows_first:
                        half_send(block, y, gy_recv.at[block], device(z, other), before)
                    ready(block, cols)
            elif op == AG_RECV:
                total_arrive(cls, block, part)
                ready(block, cols)
            elif op in (AGY_RECV, W_RECV):
                sem = gy_recv.at[block] if op == AGY_RECV else v_recv.at[via_index[field, k, side]]
                arrive(total.at[rows(block), wide_cols(other)], sem)
                ready(block, wide_cols(other))
            elif op == W_SEND:
                half_send(block, other, v_recv.at[via_index[field, k, side]], device(inward if end else outward, y))
            elif op == STAT1:
                for field in (POST, PRIOR):
                    packed = jnp.zeros((SUB, LANE), jnp.float32)
                    for b in range(nblocks):
                        packed = jnp.where(lane == b, jnp.sum(spread[field, b], axis=1, keepdims=True), packed)
                    part1[hz, field] = packed
                for b in range(1, blocks):
                    send(part1.at[hz], part1.at[hz], h_recv, {"mem": m, "hz": lax.rem(hz + b, blocks)})
                relax_load.wait()
                relax = jnp.zeros((SUB, LANE), jnp.float32)
                for level in range(levels):
                    relax = jnp.where((sub == level % SUB) & (lane == level // SUB), relax_ref[level], relax)
                state["relax"] = relax
                control_load.wait()
            elif op == STAT2:
                arrive(part1.at[pl.ds(0, blocks - 1)], h_recv)
                for field in (POST, PRIOR):
                    v = part1[0, field]
                    for b in range(1, blocks):
                        v = v + part1[b, field]
                    part2[m, field] = v
                for b in range(1, members):
                    send(part2.at[m], part2.at[m], m_recv, {"mem": lax.rem(m + b, members), "hz": hz})
            elif op == STAT3:
                arrive(part2.at[pl.ds(0, members - 1)], m_recv)
                sums = []
                for field in (POST, PRIOR):
                    v = part2[0, field]
                    for b in range(1, members):
                        v = v + part2[b, field]
                    sums.append(v)
                relax = state["relax"]
                factor = relax * (jnp.sqrt((sums[PRIOR] + eps) / (sums[POST] + eps)) - 1.0) + 1.0
                for b in range(nblocks):
                    factors[b] = jnp.broadcast_to(
                        jnp.sum(jnp.where(lane == b, factor, 0.0), axis=1, keepdims=True), (SUB, LANE))
                state["factor"] = True
            if state["factor"] and finished:
                for _ in range(2):
                    if finished:
                        finish(*finished.pop(0))
        for i, step in enumerate(order):
            do_step(i, step)
        for todo in finished:
            finish(*todo)
        if all(isinstance(cond, bool) for cond, _, _ in pending):
            tiles = sum(size for cond, _, size in pending if cond) // (SUB * LANE)
            all_sent = sent_bytes.at[pl.ds(0, tiles * SUB)]
            pltpu.make_async_copy(all_sent, all_sent, sent).wait()
        else:
            for cond, copy, _ in pending:
                when(cond, copy.wait_send)

    @pl.when(distance == 0)
    def _():
        role(plan["end"], True)

    @pl.when(distance > 0)
    def _():
        role(plan["inner"], False)


def solution(mesh):
    members, blocks = mesh.shape["mem"], mesh.shape["hz"]
    plan = PLAN if members // 2 == SHORT_LINE else LONG_PLAN

    def on_device(prior, posterior, control, relax, ocean):
        levels, columns = control.shape
        n = levels // SUB
        wide = round(columns * plan["share"] / LANE) * LANE
        parts = plan["split"]
        rest = (columns - 2 * wide) // parts
        vmem = lambda *shape: pltpu.VMEM(shape, jnp.float32)
        dma = lambda *shape: pltpu.SemaphoreType.DMA(shape)
        one = pltpu.SemaphoreType.DMA
        return pl.pallas_call(
            functools.partial(kernel, members, blocks, wide, plan),
            out_shape=pltpu.VMEM(posterior.shape, jnp.float32),
            in_specs=[pl.BlockSpec(memory_space=pltpu.HBM)] * 5,
            out_specs=pl.BlockSpec(memory_space=pltpu.VMEM),
            scratch_shapes=[
                vmem(2, levels, columns), vmem(levels, columns), pltpu.VMEM((1, columns), jnp.int32),
                pltpu.SMEM((levels,), jnp.float32), vmem(SUB, columns), vmem(levels, columns),
                vmem(2, n, SUB, wide), vmem(2, n, SUB, wide), vmem(2, n, SUB, wide), vmem(2, n, SUB, wide),
                vmem(2, n, 2, SUB, wide), vmem(2, n, parts, SUB, rest), vmem(2, n, 2, parts, SUB, rest),
                vmem(2, n, parts, SUB, rest), vmem(2, n, SUB, LANE), vmem(blocks, 2, SUB, LANE),
                vmem(members, 2, SUB, LANE), vmem(n, SUB, LANE),
                vmem(4 * levels * columns // LANE, LANE),
                dma(len(load_groups(2 * n))), one, one, one, one, dma(2, n), dma(max(1, len(plan["via"]))), dma(2, n),
                dma(2, n, parts), dma(max(1, len(plan["middle"])), parts), dma(2, n // 2, parts),
                dma(n), one, one,
            ],
            compiler_params=pltpu.CompilerParams(
                collective_id=0, has_side_effects=True, vmem_limit_bytes=60 * 2**20
            ),
        )(prior, posterior, control, relax, ocean.reshape(1, columns))

    return jax.shard_map(
        on_device,
        mesh=mesh,
        in_specs=(P("mem", None, "hz"), P("mem", None, "hz"), P(None, "hz"), P(), P("hz")),
        out_specs=P("mem", None, "hz"),
        check_vma=False,
    )
```
